32 devices in a mesh: row: 2 (over core), col: 16 (over z, y, x).
Axes of the slice: x: 2, y: 2, z: 4, core: 2. Of those that a mesh axis runs over, the one named last changes fastest.
Arguments:
- features: bfloat16 [8192, 256], P(('row', 'col')), may hold values from -6 to 6
- layer_weight: bfloat16 [256, 256], replicated, may hold values from -0.375 to 0.375
- layer_bias: float32 [256], replicated, may hold values from -3 to 3
- cotangent: bfloat16 [8192, 256], P(('row', 'col')), may hold values from -6 to 6
- tile_values: bfloat16 [1024, 256, 256], P(('row', 'col')), may hold values from -0.0625 to 0.0625
- tile_index: int32 [1024, 2], P(('row', 'col')), may hold values from -1 to 31, as said below
Outputs:
- activations: bfloat16 [8192, 256], P(('row', 'col'))
- node_grad: bfloat16 [8192, 256], P(('row', 'col'))
- weight_grad: float32 [256, 256], P(('row', 'col'))
- bias_grad: float32 [256], P(('row', 'col'))
The draws below stay inside these ranges and needn't reach their ends.
Inputs may be any that keep to these rules, and one draw needn't show every extreme that they name: `tile_index`: each pair is (I, J) with I <= J; device r * 16 + c holds only pairs whose I lies in blocks r * 16 * 1 to (r + 1) * 16 - 1 and whose J // 1 equals c modulo 16. Each pair is held by at most one slot among all devices. A device's live slots come first, its empty slots hold -1 in both entries; counts differ from device to device, and some device fills all 32 slots.
All inputs are finite; a program needn't handle non-finite values.
Results may differ from the reference program's by a relative error of at most 0.025.
Values may be sent and summed in bfloat16 or wider, within the bound.
A program may use at most 128 MiB of HBM per device.

```python
import jax
import jax.numpy as jnp
from jax import lax

TILE = 256
F = 256
BLK_DEV = 1
MAXT = 32
NBLK = 32
NODES = 8192
N_ROW = 2
N_COL = 16
DEVICES = 32


def draw_tile_index(key, part):
    row_devices = N_ROW
    column_devices = N_COL
    devices = row_devices * column_devices
    row_span = column_devices * BLK_DEV
    column_span = row_devices * BLK_DEV
    domain = row_span * column_span
    key_order = jax.random.fold_in(key, 11)
    key_count = jax.random.fold_in(key, 23)
    device_ids = jnp.arange(devices, dtype=jnp.int32)
    row_of = device_ids // column_devices
    column_of = device_ids % column_devices
    positions = jnp.arange(domain, dtype=jnp.int32)
    row_pos = positions // column_span
    column_pos = positions % column_span
    block_row = row_of[:, None] * row_span + row_pos[None, :]
    block_column = (column_pos[None, :] // BLK_DEV * column_devices + column_of[:, None]) * BLK_DEV + column_pos[None, :] % BLK_DEV
    allowed = (block_row <= block_column).astype(jnp.int32)
    scores = jax.random.randint(key_order, (devices, domain), 0, domain, dtype=jnp.int32) * domain + positions[None, :]
    scores = scores + allowed * (domain * domain)
    _, chosen = lax.top_k(scores, MAXT)
    allowed_count = jnp.sum(allowed, axis=1)
    wanted = jax.random.randint(key_count, (devices,), 1, MAXT + 1, dtype=jnp.int32)
    wanted = jnp.where(device_ids == column_devices - 1, MAXT, wanted)
    counts = jnp.minimum(wanted, allowed_count)
    slot_ids = jnp.arange(MAXT, dtype=jnp.int32)
    occupied = slot_ids[None, :] < counts[:, None]
    chosen_rows = jnp.take_along_axis(block_row, chosen, axis=1)
    chosen_columns = jnp.take_along_axis(block_column, chosen, axis=1)
    first = jnp.where(occupied, chosen_rows, -1)
    second = jnp.where(occupied, chosen_columns, -1)
    return jnp.stack([first, second], axis=-1).reshape(devices * MAXT, 2).astype(jnp.int32)


def block_scale(own_key, extent, shards, least, largest):
    def one(axis_at, shards_of):
        heights = jax.random.uniform(jax.random.fold_in(jax.random.fold_in(own_key, 6), axis_at), (shards_of,), jnp.float32, least / len(shards), largest / len(shards))
        return jnp.repeat(jnp.exp(heights), extent[axis_at] // shards_of).reshape((-1,) + (1,) * (len(extent) - axis_at - 1))

    level = one(*shards[0])
    for cut in shards[1:]:
        level = level * one(*cut)
    return level


def normal_values(key, extent, deviation, limit, split=(), kind=jnp.bfloat16):
    values = jax.random.normal(key, extent, jnp.float32) * deviation
    if len(split) > 0:
        values = block_scale(key, extent, split, -0.22, 0.18) * values
    return jnp.clip(values, min=-limit, max=limit).astype(kind)


def setup_inputs(seed: int = 0) -> dict:
    streams_of = jax.random.split(jax.random.key(seed), 7)
    return {
        "features": normal_values(streams_of[0], (NODES, F), 1.0, 6.0, ((0, 32),)),
        "layer_weight": normal_values(streams_of[1], (F, F), F ** -0.5, 0.375),
        "layer_bias": normal_values(streams_of[2], (F,), 0.5, 3.0, (), jnp.float32),
        "cotangent": normal_values(streams_of[3], (NODES, F), 1.0, 6.0, ((0, 32),)),
        "tile_values": normal_values(streams_of[4], (DEVICES * MAXT, TILE, TILE), (TILE * MAXT) ** -0.5, 0.0625, ((0, 32),)),
        "tile_index": draw_tile_index(jax.random.fold_in(streams_of[6], 71), 0),
    }


def aggregate(node_data, tile_values, tile_index):
    row_devices = N_ROW
    column_devices = N_COL
    feature_count = node_data.shape[1]
    row_span = column_devices * BLK_DEV
    column_span = row_devices * BLK_DEV
    blocks = node_data.reshape(NBLK, TILE, feature_count).astype(jnp.float32)
    device_tiles = tile_values.reshape(row_devices * column_devices, MAXT, TILE, TILE)
    device_slots = tile_index.reshape(row_devices * column_devices, MAXT, 2)
    device_ids = jnp.arange(row_devices * column_devices, dtype=jnp.int32)

    def visit_device(running, scan_item):
        row_total, column_total = running
        tile_block, slot_index, device = scan_item
        row_index = device // column_devices
        column_index = device % column_devices
        block_row = slot_index[:, 0]
        block_column = slot_index[:, 1]
        occupied = block_row >= 0
        forward_inputs = blocks[jnp.maximum(block_column, 0)]
        mirror_inputs = blocks[jnp.maximum(block_row, 0)]
        tile_floats = tile_block.astype(jnp.float32)
        forward_terms = jnp.einsum("tnm,tmf->tnf", tile_floats, forward_inputs, precision=lax.Precision.HIGHEST)
        mirror_terms = jnp.einsum("tmn,tmf->tnf", tile_floats, mirror_inputs, precision=lax.Precision.HIGHEST)
        row_slot = jnp.where(occupied, block_row - row_index * row_span, -1)
        column_slot = jnp.where(occupied, (block_column // BLK_DEV // column_devices) * BLK_DEV + block_column % BLK_DEV, -1)
        row_select = (row_slot[:, None] == jnp.arange(row_span, dtype=jnp.int32)[None, :]).astype(jnp.float32)
        column_select = (column_slot[:, None] == jnp.arange(column_span, dtype=jnp.int32)[None, :]).astype(jnp.float32)
        row_partial = jnp.einsum("ta,tnf->anf", row_select, forward_terms, precision=lax.Precision.HIGHEST)
        column_partial = jnp.einsum("tb,tnf->bnf", column_select, mirror_terms, precision=lax.Precision.HIGHEST)
        row_partial = lax.optimization_barrier(row_partial.astype(jnp.bfloat16)).astype(jnp.float32)
        column_partial = lax.optimization_barrier(column_partial.astype(jnp.bfloat16)).astype(jnp.float32)
        start = (row_index * row_span).astype(jnp.int32)
        current = lax.dynamic_slice_in_dim(row_total, start, row_span, 0)
        row_total = lax.dynamic_update_slice_in_dim(row_total, current + row_partial, start, 0)
        column_partial = column_partial.reshape(row_devices, 1, BLK_DEV, TILE, feature_count)
        current = lax.dynamic_slice_in_dim(column_total, column_index, 1, 1)
        column_total = lax.dynamic_update_slice_in_dim(column_total, current + column_partial, column_index, 1)
        return (row_total, column_total), None

    row_start = jnp.zeros((NBLK, TILE, feature_count), jnp.float32)
    column_start = jnp.zeros((row_devices, column_devices, BLK_DEV, TILE, feature_count), jnp.float32)
    (row_total, column_total), _ = lax.scan(visit_device, (row_start, column_start), (device_tiles, device_slots, device_ids))
    total = row_total.reshape(NODES, feature_count) + column_total.reshape(NODES, feature_count)
    return total.astype(jnp.bfloat16)


def reference(features, layer_weight, layer_bias, cotangent, tile_values, tile_index):
    aggregated = aggregate(features, tile_values, tile_index)
    hidden = jnp.dot(aggregated, layer_weight, preferred_element_type=jnp.float32) + layer_bias
    logistic = jax.nn.sigmoid(hidden)
    activations = (hidden * logistic).astype(jnp.bfloat16)
    derivative = logistic * (1.0 + hidden * (1.0 - logistic))
    hidden_grad = (cotangent.astype(jnp.float32) * derivative).astype(jnp.bfloat16)
    message_grad = jnp.dot(hidden_grad, layer_weight.T, preferred_element_type=jnp.float32).astype(jnp.bfloat16)
    grad_scale = NODES ** -0.5
    weight_grad = jnp.dot(aggregated.T, hidden_grad, preferred_element_type=jnp.float32) * grad_scale
    bias_grad = jnp.sum(hidden_grad.astype(jnp.float32), axis=0) * grad_scale
    node_grad = aggregate(message_grad, tile_values, tile_index)
    return activations, node_grad, weight_grad, bias_grad
```

```python
import functools

import jax
import jax.numpy as jnp
from jax import lax
from jax.experimental import pallas as pl
from jax.experimental.pallas import tpu as pltpu
from jax.sharding import PartitionSpec as P

MESH = pl.DeviceIdType.MESH
F32 = jnp.float32
BF16 = jnp.bfloat16
X, Y, LO, HI = 0, 1, 2, 3


def mm(a, b, ca, cb):
    return lax.dot_general(a, b, (((ca,), (cb,)), ((), ())), preferred_element_type=F32)


def pieces_of(tile):
    q = tile // 4
    return (
        (0, q, True, X, Y),
        (q, q, True, Y, X),
        (2 * q, 2 * q, False, X, Y),
    )


def kernel(
    n_row, n_col, scale,
    slot_ref, live_ref, feat_ref, w_ref, bias_ref, cot_ref, tiles_ref,
    act_ref, node_ref, wg_ref, bg_ref,
    G, S, R, V, M, MR, MS, TMP, WP, WX, WS, WR,
    ag_send, ag_recv, rs_send, rs_recv, v_send, v_recv, m_send, m_recv,
    wx_send, wx_recv, w_send, w_recv,
):
    tile = feat_ref.shape[0]
    nz = n_col // 4
    row = lax.axis_index("row")
    col = lax.axis_index("col")
    z = col // 4
    p = col % 4
    inner = row < n_row - 1
    pieces = pieces_of(tile)

    barrier = pltpu.get_barrier_semaphore()
    for j in range(1, n_row):
        pl.semaphore_signal(
            barrier, inc=1, device_id=(lax.rem(row + j, n_row), col), device_id_type=MESH
        )

    @pl.loop(1, n_col)
    def _(j):
        pl.semaphore_signal(
            barrier, inc=1, device_id=(row, lax.rem(col + j, n_col)), device_id_type=MESH
        )

    def flip(mask):
        return [lambda: p, lambda: p + 1 - 2 * (p % 2), lambda: p + 2 - 4 * (p // 2), lambda: 3 - p][mask]()

    bit = {X: 1, Y: 2}

    def place(mask, dz):
        return (z + dz) * 4 + flip(mask)

    def neighbour(direction):
        if direction in bit:
            return (row, place(bit[direction], 0))
        return (row, col - 4) if direction == LO else (row, col + 4)

    back = {X: X, Y: Y, LO: HI, HI: LO}

    def guarded(conds, fn):
        conds = [c for c in conds if c is not None]
        if not conds:
            fn()
        else:
            pl.when(functools.reduce(jnp.logical_and, conds))(fn)

    def aggregate(g):
        sends = []

        def gather_copy(q, src, direction):
            start, rows = pieces[q][:2]
            ref = G.at[g, src, pl.ds(start, rows)]
            return pltpu.make_async_remote_copy(
                src_ref=ref, dst_ref=ref, send_sem=ag_send.at[q, src, direction],
                recv_sem=ag_recv.at[g, q, src], device_id=neighbour(direction), device_id_type=MESH,
            )

        def gather_send(q, src, direction, conds):
            guarded(conds, lambda: gather_copy(q, src, direction).start())
            sends.append((conds, lambda: gather_copy(q, src, direction).wait_send()))

        def sum_copy(q, dst, direction):
            start, rows = pieces[q][:2]
            came = back[direction]
            return pltpu.make_async_remote_copy(
                src_ref=S.at[dst, pl.ds(start, rows)],
                dst_ref=R.at[g, came, dst, pl.ds(start, rows)],
                send_sem=rs_send.at[q, dst],
                recv_sem=rs_recv.at[g, q, came, dst],
                device_id=neighbour(direction), device_id_type=MESH,
            )

        def sum_wait(q, dst, came):
            start, rows = pieces[q][:2]
            pltpu.make_async_remote_copy(
                src_ref=S.at[dst, pl.ds(start, rows)],
                dst_ref=R.at[g, came, dst, pl.ds(start, rows)],
                send_sem=rs_send.at[q, dst],
                recv_sem=rs_recv.at[g, q, came, dst],
                device_id=neighbour(came), device_id_type=MESH,
            ).wait_recv()

        def sum_send(q, dst, direction, conds):
            guarded(conds, lambda: sum_copy(q, dst, direction).start())
            sends.append((conds, lambda: sum_copy(q, dst, direction).wait_send()))

        top, bottom = z < nz - 1, z > 0
        up_from = [(-d, [z >= d]) for d in range(1, nz)]
        down_from = [(d, [z + d < nz, inner]) for d in range(1, nz)]

        def row_copy(j):
            return pltpu.make_async_remote_copy(
                src_ref=V.at[g, row], dst_ref=V.at[g, row], send_sem=v_send.at[g, j],
                recv_sem=v_recv.at[g, row], device_id=(row - j, col), device_id_type=MESH,
            )

        for j in range(1, n_row):
            pl.when(row >= j)(lambda j=j: row_copy(j).start())
            sends.append(([row >= j], lambda j=j: row_copy(j).wait_send()))
        for q in range(len(pieces)):
            gather_send(q, col, X, [])
            gather_send(q, col, Y, [])
            gather_send(q, col, HI, [top])
            gather_send(q, col, LO, [bottom, inner])
        for k in range(n_row):
            @pl.when(k < row)
            def _(k=k):
                V[g, k] = jnp.zeros((tile, tile), BF16)

            @pl.when(k > row)
            def _(k=k):
                pltpu.make_async_remote_copy(
                    src_ref=V.at[g, k], dst_ref=V.at[g, k], send_sem=v_send.at[g, 0],
                    recv_sem=v_recv.at[g, k], device_id=(k, col), device_id_type=MESH,
                ).wait_recv()

        def load_tile(k, i):
            at = k * n_col + i
            live = jnp.full((tile, tile), live_ref[at], F32).astype(BF16)
            return tiles_ref[slot_ref[at]] * live

        @pl.loop(0, n_col)
        def _(i):
            total = mm(load_tile(0, i), V[g, 0], 1, 0)
            for k in range(1, n_row):
                total = total + mm(load_tile(k, i), V[g, k], 1, 0)
            S[i] = total.astype(BF16)

        events = []

        def add(t, conds, fn):
            events.append((t, len(events), conds, fn))

        def gather_event(t, q, mask, dz, conds, forward):
            def fn():
                src = place(mask, dz)
                start, rows = pieces[q][:2]
                ref = G.at[g, src, pl.ds(start, rows)]
                pltpu.make_async_remote_copy(
                    src_ref=ref, dst_ref=ref, send_sem=ag_send.at[q, src, X],
                    recv_sem=ag_recv.at[g, q, src], device_id=neighbour(X), device_id_type=MESH,
                ).wait_recv()
                for direction, more in forward:
                    guarded(more, lambda: gather_copy(q, src, direction).start())

            add(t, conds, fn)
            for direction, more in forward:
                sends.append((
                    conds + more,
                    lambda direction=direction: gather_copy(q, place(mask, dz), direction).wait_send(),
                ))

        def sum_event(t, q, mask, dz, conds, children, direction):
            start, rows = pieces[q][:2]

            def fn():
                dst = place(mask, dz)
                if children:
                    TMP[pl.ds(start, rows)] = S[dst, pl.ds(start, rows)].astype(F32)
                    for came, more in children:
                        def take(came=came):
                            sum_wait(q, dst, came)
                            TMP[pl.ds(start, rows)] += R[g, came, dst, pl.ds(start, rows)].astype(F32)

                        guarded(more, take)
                    if direction is not None:
                        S[dst, pl.ds(start, rows)] = TMP[pl.ds(start, rows)].astype(BF16)
                if direction is not None:
                    sum_copy(q, dst, direction).start()

            add(t, conds, fn)
            if direction is not None:
                sends.append((conds, lambda: sum_copy(q, place(mask, dz), direction).wait_send()))

        roots = []
        from_lo, from_hi = (LO, [bottom, inner]), (HI, [top])
        for q, (_, _, z_first, a, b) in enumerate(pieces):
            am, bm = bit[a], bit[b]
            every = [(0, [])] + up_from + down_from
            roots.append((q, [(a, []), (b, []), from_lo, from_hi]))
            if z_first:
                for dz, conds in up_from:
                    gather_event(-dz, q, 0, dz, conds, [(HI, [top]), (a, []), (b, [])])
                for dz, conds in down_from:
                    gather_event(dz, q, 0, dz, conds, [(LO, [bottom]), (a, []), (b, [])])
                for dz, conds in every:
                    d = abs(dz)
                    gather_event(d + 1.3, q, am, dz, conds, [(b, [])])
                    gather_event(100 + d, q, bm, dz, conds, [])
                    gather_event(101 + d, q, am | bm, dz, conds, [])
                    sum_event(-d * 0.01, q, bm, dz, conds, [], b)
                    sum_event(-d * 0.01, q, am | bm, dz, conds, [], b)
                    sum_event(2 + (nz - d) * 0.3, q, am, dz, conds, [(b, [])], a)
                for dz, conds in up_from:
                    sum_event(4 + nz + dz, q, 0, dz, conds, [(a, []), (b, []), (HI, [top])], LO)
                for dz, conds in down_from:
                    sum_event(4 + nz - dz, q, 0, dz, conds, [(a, []), (b, []), (LO, [bottom])], HI)
            else:
                spread = [(HI, [top]), (LO, [bottom, inner])]
                gather_event(1, q, am, 0, [], [(b, [])] + spread)
                gather_event(1.5, q, bm, 0, [], spread)
                gather_event(2.5, q, am | bm, 0, [], spread)
                for m in range(4):
                    for dz, conds in up_from:
                        gather_event(2.6 - dz, q, m, dz, conds, [(HI, [top])])
                        sum_event(0.8 * (nz - 1 + dz), q, m, dz, conds, [(HI, [top])], LO)
                    for dz, conds in down_from:
                        gather_event(2.6 + dz, q, m, dz, conds, [(LO, [bottom])])
                        sum_event(0.8 * (nz - 1 - dz), q, m, dz, conds, [(LO, [bottom])], HI)
                sum_event(nz + 1, q, am | bm, 0, [], [from_lo, from_hi], b)
                sum_event(nz + 1, q, bm, 0, [], [from_lo, from_hi], b)
                sum_event(nz + 2, q, am, 0, [], [(b, []), from_lo, from_hi], a)

        for _, _, conds, fn in sorted(events, key=lambda e: e[:2]):
            guarded(conds, fn)

        for k in range(n_row):
            M[k] = jnp.zeros((tile, tile), F32)

        @pl.loop(0, n_col)
        def _(i):
            @pl.when(jnp.logical_or(inner, i // 4 <= z))
            def _():
                block = G[g, i]
                for k in range(n_row):
                    @pl.when(k >= row)
                    def _(k=k):
                        M[k] += mm(block, load_tile(k, i), 1, 0)

        for k in range(n_row):
            MS[k] = M[k].astype(BF16)

        def mirror_copy(j):
            return pltpu.make_async_remote_copy(
                src_ref=MS.at[row + j], dst_ref=MR.at[g, row], send_sem=m_send.at[j],
                recv_sem=m_recv.at[g, row], device_id=(row + j, col), device_id_type=MESH,
            )

        for j in range(1, n_row):
            pl.when(row + j < n_row)(lambda j=j: mirror_copy(j).start())
            sends.append(([row + j < n_row], lambda j=j: mirror_copy(j).wait_send()))

        for q, children in roots:
            start, rows = pieces[q][:2]
            TMP[pl.ds(start, rows)] = S[col, pl.ds(start, rows)].astype(F32)
            for came, more in children:
                def take(came=came):
                    sum_wait(q, col, came)
                    TMP[pl.ds(start, rows)] += R[g, came, col, pl.ds(start, rows)].astype(F32)

                guarded(more, take)

        M[0] = MS[row].astype(F32)
        for k in range(n_row - 1):
            @pl.when(k < row)
            def _(k=k):
                pltpu.make_async_remote_copy(
                    src_ref=MS.at[k], dst_ref=MR.at[g, k], send_sem=m_send.at[0],
                    recv_sem=m_recv.at[g, k], device_id=(k, col), device_id_type=MESH,
                ).wait_recv()
                M[0] += MR[g, k].astype(F32)
        for conds, fn in sends:
            guarded(conds, fn)
        return (TMP[...] + M[0].T).astype(BF16)

    features = feat_ref[...]
    V[0, row] = features
    G[0, col] = features.astype(F32).T.astype(BF16)
    pl.semaphore_wait(barrier, n_row - 1 + n_col - 1)

    aggregated = aggregate(0)
    hidden = mm(aggregated, w_ref[...], 1, 0) + bias_ref[...]
    logistic = jax.nn.sigmoid(hidden)
    act_ref[...] = (hidden * logistic).astype(BF16)
    derivative = logistic * (1.0 + hidden * (1.0 - logistic))
    hidden_grad = (cot_ref[...].astype(F32) * derivative).astype(BF16)
    V[1, row] = mm(hidden_grad, w_ref[...], 1, 1).astype(BF16)
    G[1, col] = mm(w_ref[...], hidden_grad, 1, 1).astype(BF16)

    slice_rows = wg_ref.shape[0]
    weight_part = mm(aggregated, hidden_grad, 0, 0) * scale
    bias_part = jnp.sum(hidden_grad.astype(F32), axis=0, keepdims=True) * scale
    pad = jnp.zeros((WP.shape[2] - slice_rows - 1, tile), F32)
    for d in range(n_row * n_col):
        part = weight_part[d * slice_rows:(d + 1) * slice_rows]
        WP[d // n_col, d % n_col] = jnp.concatenate([part, bias_part, pad], axis=0).astype(BF16)

    def weight_row_copy(j):
        peer = lax.rem(row + j, n_row)
        return pltpu.make_async_remote_copy(
            src_ref=WP.at[peer], dst_ref=WX.at[j - 1], send_sem=wx_send.at[j - 1],
            recv_sem=wx_recv.at[j - 1], device_id=(peer, col), device_id_type=MESH,
        )

    for j in range(1, n_row):
        weight_row_copy(j).start()
    for j in range(1, n_row):
        weight_row_copy(j).wait()
    for i in range(n_col):
        total = WP[row, i].astype(F32)
        for j in range(1, n_row):
            total = total + WX[j - 1, i].astype(F32)
        WS[i] = total.astype(BF16)

    def weight_col_copy(j):
        peer = lax.rem(col + j, n_col)
        return pltpu.make_async_remote_copy(
            src_ref=WS.at[peer], dst_ref=WR.at[j - 1], send_sem=w_send.at[j - 1],
            recv_sem=w_recv.at[j - 1], device_id=(row, peer), device_id_type=MESH,
        )

    @pl.loop(1, n_col)
    def _(j):
        weight_col_copy(j).start()

    node_ref[...] = aggregate(1)

    @pl.loop(1, n_col)
    def _(j):
        weight_col_copy(j).wait()

    total = WS[col].astype(F32)
    for j in range(1, n_col):
        total = total + WR[j - 1].astype(F32)
    wg_ref[...] = total[:slice_rows]
    bg_ref[...] = total[slice_rows:slice_rows + 1]


def local(n_row, n_col, features, layer_weight, layer_bias, cotangent, tile_values, tile_index):
    tile, width = features.shape
    devices = n_row * n_col
    slice_rows = width // devices
    row = lax.axis_index("row")
    col = lax.axis_index("col")
    slots = tile_values.shape[0]
    first, second = tile_index[:, 0], tile_index[:, 1]
    where = jnp.where(first >= 0, second // n_col * n_col + first - row * n_col, -1)
    hit = where[None, :] == jnp.arange(devices, dtype=jnp.int32)[:, None]
    slot = jnp.sum(jnp.where(hit, jnp.arange(slots, dtype=jnp.int32)[None, :], 0), axis=1)
    live = jnp.sum(hit.astype(F32), axis=1)
    pad_rows = (slice_rows + 1 + 15) // 16 * 16
    n_piece = len(pieces_of(tile))
    dma = pltpu.SemaphoreType.DMA
    vmem = pl.BlockSpec(memory_space=pltpu.VMEM)
    smem = pl.BlockSpec(memory_space=pltpu.SMEM)
    activations, node_grad, weight_grad, bias_sum = pl.pallas_call(
        functools.partial(kernel, n_row, n_col, (tile * devices) ** -0.5),
        out_shape=(
            jax.ShapeDtypeStruct((tile, width), BF16),
            jax.ShapeDtypeStruct((tile, width), BF16),
            jax.ShapeDtypeStruct((slice_rows, width), F32),
            jax.ShapeDtypeStruct((1, width), F32),
        ),
        in_specs=[smem, smem] + [vmem] * 5,
        out_specs=(vmem,) * 4,
        scratch_shapes=[
            pltpu.VMEM((2, n_col, tile, width), BF16),
            pltpu.VMEM((n_col, tile, width), BF16),
            pltpu.VMEM((2, 4, n_col, tile, width), BF16),
            pltpu.VMEM((2, n_row, tile, width), BF16),
            pltpu.VMEM((n_row, tile, width), F32),
            pltpu.VMEM((2, n_row, tile, width), BF16),
            pltpu.VMEM((n_row, tile, width), BF16),
            pltpu.VMEM((tile, width), F32),
            pltpu.VMEM((n_row, n_col, pad_rows, width), BF16),
            pltpu.VMEM((n_row - 1, n_col, pad_rows, width), BF16),
            pltpu.VMEM((n_col, pad_rows, width), BF16),
            pltpu.VMEM((n_col - 1, pad_rows, width), BF16),
            dma((n_piece, n_col, 4)),
            dma((2, n_piece, n_col)),
            dma((n_piece, n_col)),
            dma((2, n_piece, 4, n_col)),
            dma((2, n_row)),
            dma((2, n_row)),
            dma((n_row,)),
            dma((2, n_row)),
            dma((n_row - 1,)),
            dma((n_row - 1,)),
            dma((n_col - 1,)),
            dma((n_col - 1,)),
        ],
        compiler_params=pltpu.CompilerParams(
            collective_id=0, has_side_effects=True, vmem_limit_bytes=67043328
        ),
        name="layer",
    )(slot, live, features, layer_weight, layer_bias[None, :], cotangent, tile_values)
    bias_rows = bias_sum.reshape(devices, slice_rows)
    bias_grad = lax.dynamic_index_in_dim(bias_rows, row * n_col + col, 0, keepdims=False)
    return activations, node_grad, weight_grad, bias_grad


def solution(mesh):
    n_row, n_col = mesh.shape["row"], mesh.shape["col"]
    split = P(("row", "col"), None)
    in_specs = (split, P(), P(), split, P(("row", "col"), None, None), split)
    out_specs = (split, split, split, P(("row", "col")))
    return jax.shard_map(
        functools.partial(local, n_row, n_col),
        mesh=mesh, in_specs=in_specs, out_specs=out_specs, check_vma=False,
    )
```

```python
import functools

import jax
import jax.numpy as jnp
from jax import lax
from jax.experimental import pallas as pl
from jax.experimental.pallas import tpu as pltpu
from jax.sharding import PartitionSpec as P

MESH = pl.DeviceIdType.MESH
F32 = jnp.float32
BF16 = jnp.bfloat16
X, Y, LO, HI = 0, 1, 2, 3


def mm(a, b, ca, cb):
    return lax.dot_general(a, b, (((ca,), (cb,)), ((), ())), preferred_element_type=F32)


def pieces_of(tile):
    q = tile // 4
    return (
        (0, q, True, X, Y),
        (q, q, True, Y, X),
        (2 * q, 2 * q, False, X, Y),
    )


def kernel(
    n_row, n_col, scale,
    slot_ref, live_ref, feat_ref, w_ref, bias_ref, cot_ref, tiles_ref,
    act_ref, node_ref, wg_ref, bg_ref,
    G, S, R, V, M, MR, MS, TMP, WP, WX, WS, WR,
    ag_send, ag_recv, rs_send, rs_recv, v_send, v_recv, m_send, m_recv,
    wx_send, wx_recv, w_send, w_recv,
):
    tile = feat_ref.shape[0]
    nz = n_col // 4
    row = lax.axis_index("row")
    col = lax.axis_index("col")
    z = col // 4
    p = col % 4
    inner = row < n_row - 1
    pieces = pieces_of(tile)

    barrier = pltpu.get_barrier_semaphore()
    for j in range(1, n_row):
        pl.semaphore_signal(
            barrier, inc=1, device_id=(lax.rem(row + j, n_row), col), device_id_type=MESH
        )

    @pl.loop(1, n_col)
    def _(j):
        pl.semaphore_signal(
            barrier, inc=1, device_id=(row, lax.rem(col + j, n_col)), device_id_type=MESH
        )

    def flip(mask):
        return [lambda: p, lambda: p + 1 - 2 * (p % 2), lambda: p + 2 - 4 * (p // 2), lambda: 3 - p][mask]()

    bit = {X: 1, Y: 2}

    def place(mask, dz):
        return (z + dz) * 4 + flip(mask)

    def neighbour(direction):
        if direction in bit:
            return (row, place(bit[direction], 0))
        return (row, col - 4) if direction == LO else (row, col + 4)

    back = {X: X, Y: Y, LO: HI, HI: LO}

    def guarded(conds, fn):
        conds = [c for c in conds if c is not None]
        if not conds:
            fn()
        else:
            pl.when(functools.reduce(jnp.logical_and, conds))(fn)

    def aggregate(g):
        sends = []

        def gather_copy(q, src, direction):
            start, rows = pieces[q][:2]
            ref = G.at[g, src, pl.ds(start, rows)]
            return pltpu.make_async_remote_copy(
                src_ref=ref, dst_ref=ref, send_sem=ag_send.at[q, src, direction],
                recv_sem=ag_recv.at[g, q, src], device_id=neighbour(direction), device_id_type=MESH,
            )

        def gather_send(q, src, direction, conds):
            guarded(conds, lambda: gather_copy(q, src, direction).start())
            sends.append((conds, lambda: gather_copy(q, src, direction).wait_send()))

        def sum_copy(q, dst, direction):
            start, rows = pieces[q][:2]
            came = back[direction]
            return pltpu.make_async_remote_copy(
                src_ref=S.at[dst, pl.ds(start, rows)],
                dst_ref=R.at[g, came, dst, pl.ds(start, rows)],
                send_sem=rs_send.at[q, dst],
                recv_sem=rs_recv.at[g, q, came, dst],
                device_id=neighbour(direction), device_id_type=MESH,
            )

        def sum_wait(q, dst, came):
            start, rows = pieces[q][:2]
            pltpu.make_async_remote_copy(
                src_ref=S.at[dst, pl.ds(start, rows)],
                dst_ref=R.at[g, came, dst, pl.ds(start, rows)],
                send_sem=rs_send.at[q, dst],
                recv_sem=rs_recv.at[g, q, came, dst],
                device_id=neighbour(came), device_id_type=MESH,
            ).wait_recv()

        def sum_send(q, dst, direction, conds):
            guarded(conds, lambda: sum_copy(q, dst, direction).start())
            sends.append((conds, lambda: sum_copy(q, dst, direction).wait_send()))

        top, bottom = z < nz - 1, z > 0
        up_from = [(-d, [z >= d]) for d in range(1, nz)]
        down_from = [(d, [z + d < nz, inner]) for d in range(1, nz)]

        def row_copy(j):
            return pltpu.make_async_remote_copy(
                src_ref=V.at[g, row], dst_ref=V.at[g, row], send_sem=v_send.at[g, j],
                recv_sem=v_recv.at[g, row], device_id=(row - j, col), device_id_type=MESH,
            )

        for j in range(1, n_row):
            pl.when(row >= j)(lambda j=j: row_copy(j).start())
            sends.append(([row >= j], lambda j=j: row_copy(j).wait_send()))
        for q in range(len(pieces)):
            gather_send(q, col, X, [])
            gather_send(q, col, Y, [])
            gather_send(q, col, HI, [top])
            gather_send(q, col, LO, [bottom, inner])
        for k in range(n_row):
            @pl.when(k < row)
            def _(k=k):
                V[g, k] = jnp.zeros((tile, tile), BF16)

            @pl.when(k > row)
            def _(k=k):
                pltpu.make_async_remote_copy(
                    src_ref=V.at[g, k], dst_ref=V.at[g, k], send_sem=v_send.at[g, 0],
                    recv_sem=v_recv.at[g, k], device_id=(k, col), device_id_type=MESH,
                ).wait_recv()

        def load_tile(k, i):
            at = k * n_col + i
            live = jnp.full((tile, tile), live_ref[at], F32).astype(BF16)
            return tiles_ref[slot_ref[at]] * live

        def forward_terms(y):
            @pl.loop(0, 2 * nz)
            def _(at):
                i = at // 2 * 4 + 2 * y + at % 2
                total = mm(load_tile(0, i), V[g, 0], 1, 0)
                for k in range(1, n_row):
                    total = total + mm(load_tile(k, i), V[g, k], 1, 0)
                S[i] = total.astype(BF16)

        events = []

        def add(t, conds, fn):
            events.append((t, len(events), conds, fn))

        def gather_event(t, q, mask, dz, conds, forward):
            def fn():
                src = place(mask, dz)
                start, rows = pieces[q][:2]
                ref = G.at[g, src, pl.ds(start, rows)]
                pltpu.make_async_remote_copy(
                    src_ref=ref, dst_ref=ref, send_sem=ag_send.at[q, src, X],
                    recv_sem=ag_recv.at[g, q, src], device_id=neighbour(X), device_id_type=MESH,
                ).wait_recv()
                for direction, more in forward:
                    guarded(more, lambda: gather_copy(q, src, direction).start())

            add(t, conds, fn)
            for direction, more in forward:
                sends.append((
                    conds + more,
                    lambda direction=direction: gather_copy(q, place(mask, dz), direction).wait_send(),
                ))

        def sum_event(t, q, mask, dz, conds, children, direction):
            start, rows = pieces[q][:2]

            def fn():
                dst = place(mask, dz)
                if children:
                    TMP[pl.ds(start, rows)] = S[dst, pl.ds(start, rows)].astype(F32)
                    for came, more in children:
                        def take(came=came):
                            sum_wait(q, dst, came)
                            TMP[pl.ds(start, rows)] += R[g, came, dst, pl.ds(start, rows)].astype(F32)

                        guarded(more, take)
                    if direction is not None:
                        S[dst, pl.ds(start, rows)] = TMP[pl.ds(start, rows)].astype(BF16)
                if direction is not None:
                    sum_copy(q, dst, direction).start()

            add(t, conds, fn)
            if direction is not None:
                sends.append((conds, lambda: sum_copy(q, place(mask, dz), direction).wait_send()))

        roots = []
        from_lo, from_hi = (LO, [bottom, inner]), (HI, [top])
        for q, (_, _, z_first, a, b) in enumerate(pieces):
            am, bm = bit[a], bit[b]
            every = [(0, [])] + up_from + down_from
            roots.append((q, [(a, []), (b, []), from_lo, from_hi]))
            if z_first:
                for dz, conds in up_from:
                    gather_event(-dz, q, 0, dz, conds, [(HI, [top]), (a, []), (b, [])])
                for dz, conds in down_from:
                    gather_event(dz, q, 0, dz, conds, [(LO, [bottom]), (a, []), (b, [])])
                for dz, conds in every:
                    d = abs(dz)
                    gather_event(d + 1.3, q, am, dz, conds, [(b, [])])
                    gather_event(100 + d if d else 3.8, q, bm, dz, conds, [])
                    gather_event(100.1 + d if d else 3.85, q, am | bm, dz, conds, [])
                    early = -1 if b == Y else 0
                    sum_event(early - d * 0.01, q, bm, dz, conds, [], b)
                    sum_event(early - d * 0.01, q, am | bm, dz, conds, [], b)
                    sum_event(2 + (nz - d) * 0.3, q, am, dz, conds, [(b, [])], a)
                for dz, conds in up_from:
                    sum_event(4 + nz + dz, q, 0, dz, conds, [(a, []), (b, []), (HI, [top])], LO)
                for dz, conds in down_from:
                    sum_event(4 + nz - dz, q, 0, dz, conds, [(a, []), (b, []), (LO, [bottom])], HI)
            else:
                spread = [(HI, [top]), (LO, [bottom, inner])]
                gather_event(1, q, am, 0, [], [(b, [])] + spread)
                gather_event(1.5, q, bm, 0, [], spread)
                gather_event(2.5, q, am | bm, 0, [], spread)
                for m in range(4):
                    for dz, conds in up_from:
                        gather_event(2.6 - dz, q, m, dz, conds, [(HI, [top])])
                        sum_event(0.8 * (nz - 1 + dz), q, m, dz, conds, [(HI, [top])], LO)
                    for dz, conds in down_from:
                        gather_event(2.6 + dz, q, m, dz, conds, [(LO, [bottom])])
                        sum_event(0.8 * (nz - 1 - dz), q, m, dz, conds, [(LO, [bottom])], HI)
                sum_event(nz + 1, q, am | bm, 0, [], [from_lo, from_hi], b)
                sum_event(nz + 1, q, bm, 0, [], [from_lo, from_hi], b)
                sum_event(nz + 2, q, am, 0, [], [(b, []), from_lo, from_hi], a)

        def mirror_terms(dz):
            @pl.loop(0, 4 * n_row)
            def _(at):
                i = (z + dz) * 4 + at // n_row
                k = at % n_row

                @pl.when(k >= row)
                def _():
                    M[k] += mm(G[g, i], load_tile(k, i), 1, 0)

        for dz, conds in [(0, [])] + up_from + down_from:
            add(100.5 + abs(dz) if dz else 3.9, conds, lambda dz=dz: mirror_terms(dz))

        for k in range(n_row):
            M[k] = jnp.zeros((tile, tile), F32)
        forward_terms(1 - p // 2)
        add(-0.5, [], lambda: forward_terms(p // 2))
        for _, _, conds, fn in sorted(events, key=lambda e: e[:2]):
            guarded(conds, fn)

        for k in range(n_row):
            MS[k] = M[k].astype(BF16)

        def mirror_copy(j):
            return pltpu.make_async_remote_copy(
                src_ref=MS.at[row + j], dst_ref=MR.at[g, row], send_sem=m_send.at[j],
                recv_sem=m_recv.at[g, row], device_id=(row + j, col), device_id_type=MESH,
            )

        for j in range(1, n_row):
            pl.when(row + j < n_row)(lambda j=j: mirror_copy(j).start())
            sends.append(([row + j < n_row], lambda j=j: mirror_copy(j).wait_send()))

        for q, children in roots:
            start, rows = pieces[q][:2]
            TMP[pl.ds(start, rows)] = S[col, pl.ds(start, rows)].astype(F32)
            for came, more in children:
                def take(came=came):
                    sum_wait(q, col, came)
                    TMP[pl.ds(start, rows)] += R[g, came, col, pl.ds(start, rows)].astype(F32)

                guarded(more, take)

        M[0] = MS[row].astype(F32)
        for k in range(n_row - 1):
            @pl.when(k < row)
            def _(k=k):
                pltpu.make_async_remote_copy(
                    src_ref=MS.at[k], dst_ref=MR.at[g, k], send_sem=m_send.at[0],
                    recv_sem=m_recv.at[g, k], device_id=(k, col), device_id_type=MESH,
                ).wait_recv()
                M[0] += MR[g, k].astype(F32)
        for conds, fn in sends:
            guarded(conds, fn)
        return (TMP[...] + M[0].T).astype(BF16)

    features = feat_ref[...]
    V[0, row] = features
    G[0, col] = features.astype(F32).T.astype(BF16)
    pl.semaphore_wait(barrier, n_row - 1 + n_col - 1)

    aggregated = aggregate(0)
    hidden = mm(aggregated, w_ref[...], 1, 0) + bias_ref[...]
    logistic = jax.nn.sigmoid(hidden)
    act_ref[...] = (hidden * logistic).astype(BF16)
    derivative = logistic * (1.0 + hidden * (1.0 - logistic))
    hidden_grad = (cot_ref[...].astype(F32) * derivative).astype(BF16)
    V[1, row] = mm(hidden_grad, w_ref[...], 1, 1).astype(BF16)
    G[1, col] = mm(w_ref[...], hidden_grad, 1, 1).astype(BF16)

    slice_rows = wg_ref.shape[0]
    weight_part = mm(aggregated, hidden_grad, 0, 0) * scale
    bias_part = jnp.sum(hidden_grad.astype(F32), axis=0, keepdims=True) * scale
    pad = jnp.zeros((WP.shape[2] - slice_rows - 1, tile), F32)
    for d in range(n_row * n_col):
        part = weight_part[d * slice_rows:(d + 1) * slice_rows]
        WP[d // n_col, d % n_col] = jnp.concatenate([part, bias_part, pad], axis=0).astype(BF16)

    def weight_row_copy(j):
        peer = lax.rem(row + j, n_row)
        return pltpu.make_async_remote_copy(
            src_ref=WP.at[peer], dst_ref=WX.at[j - 1], send_sem=wx_send.at[j - 1],
            recv_sem=wx_recv.at[j - 1], device_id=(peer, col), device_id_type=MESH,
        )

    for j in range(1, n_row):
        weight_row_copy(j).start()
    for j in range(1, n_row):
        weight_row_copy(j).wait()
    for i in range(n_col):
        total = WP[row, i].astype(F32)
        for j in range(1, n_row):
            total = total + WX[j - 1, i].astype(F32)
        WS[i] = total.astype(BF16)

    def weight_col_copy(j):
        peer = lax.rem(col + j, n_col)
        return pltpu.make_async_remote_copy(
            src_ref=WS.at[peer], dst_ref=WR.at[j - 1], send_sem=w_send.at[j - 1],
            recv_sem=w_recv.at[j - 1], device_id=(row, peer), device_id_type=MESH,
        )

    @pl.loop(1, n_col)
    def _(j):
        weight_col_copy(j).start()

    node_ref[...] = aggregate(1)

    @pl.loop(1, n_col)
    def _(j):
        weight_col_copy(j).wait()

    total = WS[col].astype(F32)
    for j in range(1, n_col):
        total = total + WR[j - 1].astype(F32)
    wg_ref[...] = total[:slice_rows]
    bg_ref[...] = total[slice_rows:slice_rows + 1]


def local(n_row, n_col, features, layer_weight, layer_bias, cotangent, tile_values, tile_index):
    tile, width = features.shape
    devices = n_row * n_col
    slice_rows = width // devices
    row = lax.axis_index("row")
    col = lax.axis_index("col")
    slots = tile_values.shape[0]
    first, second = tile_index[:, 0], tile_index[:, 1]
    where = jnp.where(first >= 0, second // n_col * n_col + first - row * n_col, -1)
    hit = where[None, :] == jnp.arange(devices, dtype=jnp.int32)[:, None]
    slot = jnp.sum(jnp.where(hit, jnp.arange(slots, dtype=jnp.int32)[None, :], 0), axis=1)
    live = jnp.sum(hit.astype(F32), axis=1)
    pad_rows = (slice_rows + 1 + 15) // 16 * 16
    n_piece = len(pieces_of(tile))
    dma = pltpu.SemaphoreType.DMA
    vmem = pl.BlockSpec(memory_space=pltpu.VMEM)
    smem = pl.BlockSpec(memory_space=pltpu.SMEM)
    activations, node_grad, weight_grad, bias_sum = pl.pallas_call(
        functools.partial(kernel, n_row, n_col, (tile * devices) ** -0.5),
        out_shape=(
            jax.ShapeDtypeStruct((tile, width), BF16),
            jax.ShapeDtypeStruct((tile, width), BF16),
            jax.ShapeDtypeStruct((slice_rows, width), F32),
            jax.ShapeDtypeStruct((1, width), F32),
        ),
        in_specs=[smem, smem] + [vmem] * 5,
        out_specs=(vmem,) * 4,
        scratch_shapes=[
            pltpu.VMEM((2, n_col, tile, width), BF16),
            pltpu.VMEM((n_col, tile, width), BF16),
            pltpu.VMEM((2, 4, n_col, tile, width), BF16),
            pltpu.VMEM((2, n_row, tile, width), BF16),
            pltpu.VMEM((n_row, tile, width), F32),
            pltpu.VMEM((2, n_row, tile, width), BF16),
            pltpu.VMEM((n_row, tile, width), BF16),
            pltpu.VMEM((tile, width), F32),
            pltpu.VMEM((n_row, n_col, pad_rows, width), BF16),
            pltpu.VMEM((n_row - 1, n_col, pad_rows, width), BF16),
            pltpu.VMEM((n_col, pad_rows, width), BF16),
            pltpu.VMEM((n_col - 1, pad_rows, width), BF16),
            dma((n_piece, n_col, 4)),
            dma((2, n_piece, n_col)),
            dma((n_piece, n_col)),
            dma((2, n_piece, 4, n_col)),
            dma((2, n_row)),
            dma((2, n_row)),
            dma((n_row,)),
            dma((2, n_row)),
            dma((n_row - 1,)),
            dma((n_row - 1,)),
            dma((n_col - 1,)),
            dma((n_col - 1,)),
        ],
        compiler_params=pltpu.CompilerParams(
            collective_id=0, has_side_effects=True, vmem_limit_bytes=67043328
        ),
        name="layer",
    )(slot, live, features, layer_weight, layer_bias[None, :], cotangent, tile_values)
    bias_rows = bias_sum.reshape(devices, slice_rows)
    bias_grad = lax.dynamic_index_in_dim(bias_rows, row * n_col + col, 0, keepdims=False)
    return activations, node_grad, weight_grad, bias_grad


def solution(mesh):
    n_row, n_col = mesh.shape["row"], mesh.shape["col"]
    split = P(("row", "col"), None)
    in_specs = (split, P(), P(), split, P(("row", "col"), None, None), split)
    out_specs = (split, split, split, P(("row", "col")))
    return jax.shard_map(
        functools.partial(local, n_row, n_col),
        mesh=mesh, in_specs=in_specs, out_specs=out_specs, check_vma=False,
    )
```
